512 devices in a mesh: section: 16 (over y, core), dp: 32 (over x, z).
Axes of the slice: x: 4, y: 8, z: 8, core: 2. Of those that a mesh axis runs over, the one named last changes fastest.
Arguments:
- patch_tokens: bfloat16 [4, 32, 196, 1280], P(None, 'dp'), may hold values from -24 to 24
- visible: int32 [4, 32, 98], P(None, 'dp'), may hold values from 0 to 195, as said below
- keep_mask: int32 [4, 32, 98], P(None, 'dp'), may hold values from 0 to 1, as said below
- lengths: int32 [4], replicated, may hold values from 49 to 98
- qkv_weight: bfloat16 [16, 1280, 1920], P('section', 'dp'), may hold values from -4 to 4
- out_weight: bfloat16 [16, 640, 1280], P('section', 'dp'), may hold values from -0.25 to 0.25
- norm_gain: bfloat16 [16, 1280], P('section'), may hold values from 0.099609375 to 1.8984375
- targets: bfloat16 [16, 4, 32, 98, 1280], P('section', None, 'dp'), may hold values from -12 to 12
Outputs:
- hidden_states: bfloat16 [16, 4, 32, 98, 1280], P('section', None, 'dp')
- token_loss: float32 [4, 32, 98], P(None, 'dp')
- loss: float32 [4], replicated
The draws below stay inside these ranges and needn't reach their ends.
Inputs may be any that keep to these rules, and one draw needn't show every extreme that they name: `visible`: the 98 entries of one image are different patch numbers. `keep_mask`: slot 0 of every image is 1.
All inputs are finite; a program needn't handle non-finite values.
Results may differ from the reference program's by a relative error of at most 0.019.
Values may be sent and summed in bfloat16 or wider, within the bound.
A program may use at most 128 MiB of HBM per device.

```python
import jax
import jax.numpy as jnp
from jax import lax

D = 1280
HEADS = 8
HDIM = 80
NPATCH = 196
BMIN = 49
BMAX = 98
MICRO = 4
IMAGES = 32
LAYERS = 16


def draw_visible(key, part):
    row_keys = jax.random.split(key, MICRO * IMAGES)
    shuffled = jax.vmap(lambda one_key: jax.random.permutation(one_key, NPATCH))(row_keys)
    return shuffled[:, :BMAX].reshape(MICRO, IMAGES, BMAX).astype(jnp.int32)


def draw_keep_mask(key, part):
    ticket = jax.random.randint(key, (MICRO, IMAGES, BMAX), 0, 1000)
    image_pos = jnp.arange(IMAGES, dtype=jnp.int32)
    threshold = 300 + 600 * image_pos // max(IMAGES - 1, 1)
    keep_flags = (ticket < threshold[None, :, None]).astype(jnp.int32)
    leading = jnp.arange(BMAX, dtype=jnp.int32) == 0
    return jnp.where(leading[None, None, :], 1, keep_flags).astype(jnp.int32)


def patch_values(key):
    patch_key = jax.random.fold_in(key, 21)
    shape = (MICRO, IMAGES, NPATCH, D)
    values = jax.random.truncated_normal(patch_key, -6.0, 6.0, shape, jnp.float32)
    return jnp.clip(values, -24.0, 24.0).astype(jnp.bfloat16)


def draw_patch_tokens(key, part):
    return patch_values(key)


def draw_qkv_weight(key, part):
    base = jax.random.truncated_normal(key, -4.0, 4.0, (LAYERS, D, 3, HEADS, HDIM), jnp.float32) * D ** (-0.5)
    base = jnp.clip(base, -4.0, 4.0)
    return base.reshape(LAYERS, D, 3 * HEADS * HDIM).astype(jnp.bfloat16)


def draw_targets(key, part):
    shape = (LAYERS, MICRO, IMAGES, BMAX, D)
    tokens = patch_values(key)
    chosen = draw_visible(key, part)
    gathered = jnp.take_along_axis(tokens, chosen[:, :, :, None], axis=2).astype(jnp.float32)
    row_mean = jnp.mean(gathered, -1, keepdims=True)
    centered = gathered - row_mean
    variance = jnp.mean(centered * centered, -1, keepdims=True)
    base = centered * lax.rsqrt(variance + 1e-06)
    layer_pos = jnp.arange(LAYERS, dtype=jnp.float32) / max(LAYERS - 1, 1)
    image_pos = jnp.arange(IMAGES, dtype=jnp.float32) / max(IMAGES - 1, 1)
    noise_key = jax.random.fold_in(key, 31)
    noise = jax.random.truncated_normal(noise_key, -4.0, 4.0, shape, jnp.float32)
    layer_scale = 0.25 * (1.0 + 2.0 * layer_pos)
    image_scale = 1.0 + image_pos
    noise = noise * layer_scale[:, None, None, None, None] * image_scale[None, None, :, None, None]
    values = base[None] + noise
    return jnp.clip(values, -12.0, 12.0).astype(jnp.bfloat16)


def touch_ends(drawn, stream_key, least, high):
    shape = drawn.shape
    spot = [jax.random.randint(jax.random.fold_in(stream_key, axis), (), 0, shape[axis]) for axis in range(len(shape))]
    drawn = drawn.at[tuple(spot)].set(least)
    longest = shape.index(max(shape))
    spot[longest] = (spot[longest] + 1) % shape[longest]
    return drawn.at[tuple(spot)].set(high)


def level_of(stream_key, shape, cuts, least, high):
    def one(position, blocks):
        steps = jax.random.uniform(jax.random.fold_in(jax.random.fold_in(stream_key, 6), position), (blocks,), jnp.float32, least / len(cuts), high / len(cuts))
        return jnp.repeat(jnp.exp(steps), shape[position] // blocks).reshape((-1,) + (1,) * (len(shape) - position - 1))

    factor_of = one(*cuts[0])
    for cut in cuts[1:]:
        factor_of = factor_of * one(*cut)
    return factor_of


def normal_values(own_key, shape, width, most, cuts=(), held_as=jnp.bfloat16):
    drawn = jax.random.normal(own_key, shape, jnp.float32) * width
    if len(cuts) > 0:
        drawn = level_of(own_key, shape, cuts, -0.22, 0.18) * drawn
    return jnp.clip(drawn, min=-most, max=most).astype(held_as)


def setup_inputs(seed: int = 0) -> dict:
    keys = jax.random.split(jax.random.key(seed), 9)
    return {
        "patch_tokens": draw_patch_tokens(jax.random.fold_in(keys[8], 71), 0),
        "visible": draw_visible(jax.random.fold_in(keys[8], 71), 0),
        "keep_mask": draw_keep_mask(jax.random.fold_in(keys[8], 71), 0),
        "lengths": touch_ends(jax.random.randint(keys[3], (MICRO,), BMIN, BMAX + 1), jax.random.fold_in(keys[3], 1), BMIN, BMAX).astype(jnp.int32),
        "qkv_weight": draw_qkv_weight(jax.random.fold_in(keys[8], 71), 0),
        "out_weight": normal_values(keys[5], (LAYERS, HEADS * HDIM, D), (HEADS * HDIM) ** -0.5, 0.25, ((0, 16), (1, 32))),
        "norm_gain": jnp.clip(1.0 + 0.18 * jax.random.normal(keys[6], (LAYERS, D), jnp.float32), 0.099609375, 1.8984375).astype(jnp.bfloat16),
        "targets": draw_targets(jax.random.fold_in(keys[8], 71), 0),
    }


def norm_rows(values):
    row_mean = lax.optimization_barrier(jnp.mean(values, -1, keepdims=True))
    centered = values - row_mean
    variance = lax.optimization_barrier(jnp.mean(centered * centered, -1, keepdims=True))
    return centered * lax.rsqrt(variance + 1e-06)

def encoder_layer(tokens_now, live_rows, norm_scale, w_qkv, w_out):
    images, row_count, model_width = tokens_now.shape
    normed = (norm_rows(tokens_now.astype(jnp.float32)) * norm_scale).astype(jnp.bfloat16)
    projections = jnp.dot(normed.reshape(images * row_count, model_width), w_qkv, preferred_element_type=jnp.float32).astype(jnp.bfloat16)
    projections = projections.reshape(images, row_count, 3, HEADS, HDIM)
    queries = projections[:, :, 0].astype(jnp.float32)
    key_rows = projections[:, :, 1].astype(jnp.float32)
    value_rows = projections[:, :, 2].astype(jnp.float32)
    scores = jnp.einsum('iqhe,ikhe->ihqk', queries, key_rows) * HDIM ** (-0.5)
    scores = jnp.where(live_rows[:, None, None, :], scores, -1e+30)
    row_max = lax.optimization_barrier(jnp.max(scores, -1, keepdims=True))
    weights = jnp.exp(scores - row_max)
    probabilities = (weights / lax.optimization_barrier(jnp.sum(weights, -1, keepdims=True))).astype(jnp.bfloat16)
    context = jnp.einsum('ihqk,ikhe->iqhe', probabilities.astype(jnp.float32), value_rows).astype(jnp.bfloat16)
    projected = jnp.dot(context.reshape(images * row_count, HEADS * HDIM), w_out, preferred_element_type=jnp.float32)
    return (tokens_now.astype(jnp.float32) + projected.reshape(images, row_count, model_width)).astype(jnp.bfloat16)

def reference(patch_tokens, visible, keep_mask, lengths, qkv_weight, out_weight, norm_gain, targets):
    positions = jnp.arange(BMAX, dtype=jnp.int32)
    live = (positions[None, None, :] < lengths[:, None, None]) & (keep_mask == 1)
    tokens_now = jnp.take_along_axis(patch_tokens, visible[:, :, :, None], axis=2)
    tokens_now = tokens_now.reshape(MICRO * IMAGES, BMAX, D)
    flat_live = live.reshape(MICRO * IMAGES, BMAX)
    token_error = jnp.zeros((MICRO * IMAGES, BMAX), jnp.float32)
    layer_outputs = []
    for layer_index in range(LAYERS):
        tokens_now = encoder_layer(tokens_now, flat_live, norm_gain[layer_index].astype(jnp.float32), qkv_weight[layer_index], out_weight[layer_index])
        masked = jnp.where(flat_live[:, :, None], tokens_now, jnp.zeros_like(tokens_now))
        layer_outputs.append(masked.reshape(MICRO, IMAGES, BMAX, D))
        deviation = norm_rows(tokens_now.astype(jnp.float32)) - targets[layer_index].reshape(MICRO * IMAGES, BMAX, D).astype(jnp.float32)
        token_error = token_error + jnp.where(flat_live, lax.optimization_barrier(jnp.mean(deviation * deviation, -1)), jnp.float32(0.0))
    token_loss = token_error.reshape(MICRO, IMAGES, BMAX)
    count = lax.optimization_barrier(jnp.sum(live.astype(jnp.float32), axis=(1, 2)))
    loss = lax.optimization_barrier(jnp.sum(token_loss, axis=(1, 2))) / count
    return (jnp.stack(layer_outputs), token_loss, loss)
```

```python
import functools

import jax
import jax.numpy as jnp
from jax import lax
from jax.experimental import pallas as pl
from jax.experimental.pallas import tpu as pltpu
from jax.sharding import PartitionSpec as P

HDIM = 80
SPLIT = 48
X = 4


def normalised(values):
    row_mean = jnp.mean(values, -1, keepdims=True)
    centered = values - row_mean
    variance = jnp.mean(centered * centered, -1, keepdims=True)
    return centered * lax.rsqrt(variance + 1e-06)


def gather_plan(xs, zs):
    waiting = []

    def one_way(part, where):
        out = []
        if part == 0:
            first, second = (zs, xs)
        else:
            first, second = (xs, zs)
        flows = {1: first // 2, -1: first - 1 - first // 2}
        cross = {1: second // 2, -1: second - 1 - second // 2}
        return (flows, cross)

    times = {}
    links = {}
    heap = []
    cost = {0: 2.6, 1: 1.8}

    def link_of(key, way, ring):
        part, f, s = key
        if ring == 0:
            sign = way
        else:
            sign = way if f % 2 == 0 else -way
        dim = ("z", "x")[part] if ring == 0 else ("x", "z")[part]
        return (dim, sign)

    def push(key, way, ring, ready):
        heap.append((ready, len(heap), key, way, ring))

    def arrived(key, ready):
        part, f, s = key
        flows, cross = one_way(part, None)
        if s == 0:
            for way in (1, -1):
                if (f == 0 or (f > 0) == (way > 0)) and abs(f) < flows[way]:
                    push((part, f + way, 0), way, 0, ready)
            for way in (1, -1):
                push((part, f, way), way, 1, ready + 0.01)
        else:
            way = 1 if s > 0 else -1
            if abs(s) < cross[way]:
                push((part, f, s + way), way, 1, ready)

    arrived((0, 0, 0), 0.0)
    arrived((1, 0, 0), 0.0)
    while heap:
        heap.sort()
        ready, _, key, way, ring = heap.pop(0)
        link = link_of(key, way, ring)
        begin = max(ready, links.get(link, 0.0))
        links[link] = begin + cost[key[0]]
        times[key] = begin + cost[key[0]] + 1.6
        arrived(key, times[key] + 0.1)
    return sorted(times, key=lambda key: times[key])


def kernel(
    dims,
    lengths_ref,
    visible_ref,
    keep_ref,
    wq_ref,
    wo_ref,
    gain_ref,
    patch_hbm,
    target_hbm,
    hidden_hbm,
    token_ref,
    loss_ref,
    slabs,
    wqkv,
    wout,
    patch,
    target,
    xin,
    yout,
    hid,
    qkv,
    ctx,
    err_in,
    err_out,
    live_rows,
    tl,
    part_own,
    part_mid,
    slots_x,
    slots_z,
    load_sem,
    hid_sem,
    own_recv,
    send_first,
    send_second,
    x_send,
    x_recv,
    e_send,
    e_recv,
    t_send,
    t_recv,
    rx_send,
    rx_recv,
    rz_send,
    rz_recv,
):
    sections, xs, zs, micro, rows, model, heads = dims
    width = heads * HDIM
    patches = patch.shape[1]
    section = lax.axis_index("section")
    me = lax.axis_index("dp")
    mx, mz = me // zs, me % zs
    last = sections - 1
    ring = {"x": xs, "z": zs}

    def at(x, z):
        return lax.rem(x + 2 * xs, xs) * zs + lax.rem(z + 2 * zs, zs)

    barrier = pltpu.get_barrier_semaphore()
    for there in (at(mx + 1, mz), at(mx - 1, mz), at(mx, mz + 1), at(mx, mz - 1)):
        pl.semaphore_signal(barrier, inc=1, device_id={"dp": there})

    @pl.when(section > 0)
    def _():
        pl.semaphore_signal(barrier, inc=1, device_id={"section": section - 1})

    @pl.when(section < last)
    def _():
        pl.semaphore_signal(barrier, inc=1, device_id={"section": section + 1})

    target_load = pltpu.make_async_copy(target_hbm, target, load_sem.at[0])
    target_load.start()
    patch_load = pltpu.make_async_copy(patch_hbm, patch, load_sem.at[1])
    patch_load.start()

    half = model // 2
    w = wq_ref[...].astype(jnp.float32)
    o = wo_ref[...].astype(jnp.float32)
    left = jnp.concatenate(
        [
            w[:, :half],
            w[0:8, model : model + half],
            w[16:24, model : model + half],
            w[32:40, model : model + half],
            o[0:16, :half],
        ],
        axis=0,
    )
    right = jnp.concatenate(
        [
            w[:, half:model],
            w[8:16, model : model + half],
            w[24:32, model : model + half],
            jnp.concatenate([o[16:20, :half], o[16:20, half:]], axis=0),
            o[0:16, half:],
        ],
        axis=0,
    )
    slabs[me, :, 0:half] = left.astype(jnp.bfloat16)
    slabs[me, :, half:model] = right.astype(jnp.bfloat16)

    pl.semaphore_wait(barrier, 4 + jnp.minimum(section, 1) + jnp.minimum(last - section, 1))

    def sign(c):
        return 1 - 2 * lax.rem(c + 2 * xs * zs, 2)

    def cut(origin, part):
        if part == 0:
            return slabs.at[origin, pl.ds(0, SPLIT)]
        return slabs.at[origin, pl.ds(SPLIT, slabs.shape[1] - SPLIT)]

    sends = []

    def place(key, receiver):
        part, f, s = key
        if part == 0:
            way1 = sign(mx)
            if receiver:
                oz = mz - f * way1
                way2 = sign(oz)
                return at(mx - s * way2, oz), None
        else:
            way1 = sign(mz)
            if receiver:
                ox = mx - f * way1
                way2 = sign(ox)
                return at(ox, mz - s * way2), None

    def send(key):
        part, f, s = key
        step = 1 if (s > 0 or (s == 0 and f > 0)) else -1
        if part == 0:
            way1 = sign(mx)
            if s == 0:
                origin = at(mx, mz - (f - step) * way1)
                there = at(mx, mz + step * way1)
                sem = send_first.at[part, f + zs]
            else:
                oz = mz - f * way1
                way2 = sign(oz)
                origin = at(mx - (s - step) * way2, oz)
                there = at(mx + step * way2, mz)
                sem = send_second.at[part, f + zs, s + zs]
        else:
            way1 = sign(mz)
            if s == 0:
                origin = at(mx - (f - step) * way1, mz)
                there = at(mx + step * way1, mz)
                sem = send_first.at[part, f + zs]
            else:
                ox = mx - f * way1
                way2 = sign(ox)
                origin = at(ox, mz - (s - step) * way2)
                there = at(mx, mz + step * way2)
                sem = send_second.at[part, f + zs, s + zs]
        copy = pltpu.make_async_remote_copy(
            src_ref=cut(origin, part),
            dst_ref=cut(origin, part),
            send_sem=sem,
            recv_sem=own_recv.at[part, origin],
            device_id={"dp": there},
        )
        copy.start()
        sends.append(copy)

    def after(key):
        part, f, s = key
        first, second = (zs, xs) if part == 0 else (xs, zs)
        flows = {1: first // 2, -1: first - 1 - first // 2}
        cross = {1: second // 2, -1: second - 1 - second // 2}
        if s == 0:
            for way in (1, -1):
                if (f == 0 or (f > 0) == (way > 0)) and abs(f) < flows[way]:
                    send((part, f + way, 0))
            for way in (1, -1):
                send((part, f, way))
        else:
            way = 1 if s > 0 else -1
            if abs(s) < cross[way]:
                send((part, f, s + way))

    plan = gather_plan(xs, zs)
    after((0, 0, 0))
    after((1, 0, 0))

    lane = lax.broadcasted_iota(jnp.int32, (rows, 128), 1)
    sub = lax.broadcasted_iota(jnp.int32, (rows, 128), 0)
    eye = lane == sub
    slot = lax.broadcasted_iota(jnp.int32, (1, rows), 1)
    for m in range(micro):
        keep = keep_ref[m : m + 1, :]
        alive = jnp.where((slot < lengths_ref[m]) & (keep == 1), 1.0, 0.0)
        live_rows[m, :, 0:rows] = jnp.broadcast_to(alive, (8, rows))

    def column(row):
        return jnp.sum(jnp.where(eye[:, :rows], row, 0.0), axis=1, keepdims=True)

    patch_load.wait()

    @pl.when(section == 0)
    def _():
        for m in range(micro):
            chosen = column(visible_ref[m : m + 1, :].astype(jnp.float32))
            spot = lax.broadcasted_iota(jnp.int32, (rows, patches), 1).astype(jnp.float32)
            pick = jnp.where(spot == chosen, 1.0, 0.0).astype(jnp.bfloat16)
            xin[m] = jnp.dot(pick, patch[m], preferred_element_type=jnp.float32).astype(
                jnp.bfloat16
            )
            err_in[m] = jnp.zeros(err_in.shape[1:], jnp.float32)

    for key in plan:
        part = key[0]
        origin, _ = place(key, True)
        pltpu.make_async_remote_copy(
            src_ref=cut(origin, part),
            dst_ref=cut(origin, part),
            send_sem=send_first.at[part, 0],
            recv_sem=own_recv.at[part, origin],
            device_id={"dp": me},
        ).wait_recv()
        after(key)

    @pl.loop(0, xs * zs // 4)
    def _(g):
        r160 = pl.multiple_of(g * 160, 16)
        r80 = pl.multiple_of(g * 80, 16)
        for c in range(0, half, 128):
            a = [slabs[g * 4 + j, :, c : c + 128].astype(jnp.float32) for j in range(4)]
            b = [
                slabs[g * 4 + j, :, half + c : half + c + 128].astype(jnp.float32)
                for j in range(4)
            ]
            qk0 = jnp.concatenate([t[0:40] for t in a], axis=0)
            qk1 = jnp.concatenate([t[0:40] for t in b], axis=0)
            val = []
            o0 = []
            o1 = []
            for t, u in zip(a, b):
                val += [t[40:48], u[40:48], t[48:56], u[48:56], t[56:64]]
                o0 += [t[64:80], u[56:60]]
                o1 += [u[64:80], u[60:64]]
            wqkv[pl.ds(r160, 160), c : c + 128] = qk0.astype(jnp.bfloat16)
            wqkv[pl.ds(r160, 160), half + c : half + c + 128] = qk1.astype(jnp.bfloat16)
            wqkv[pl.ds(r160, 160), model + c : model + c + 128] = jnp.concatenate(
                val, axis=0
            ).astype(jnp.bfloat16)
            wout[pl.ds(r80, 80), c : c + 128] = jnp.concatenate(o0, axis=0).astype(jnp.bfloat16)
            wout[pl.ds(r80, 80), half + c : half + c + 128] = jnp.concatenate(
                o1, axis=0
            ).astype(jnp.bfloat16)

    target_load.wait()
    gain = gain_ref[...].astype(jnp.float32)
    to_next = jnp.minimum(section + 1, last)

    def token_copy(m):
        return pltpu.make_async_remote_copy(
            src_ref=yout.at[m],
            dst_ref=xin.at[m],
            send_sem=x_send.at[m],
            recv_sem=x_recv.at[m],
            device_id={"section": to_next},
        )

    def error_copy(m):
        return pltpu.make_async_remote_copy(
            src_ref=err_out.at[m],
            dst_ref=err_in.at[m],
            send_sem=e_send.at[m],
            recv_sem=e_recv.at[m],
            device_id={"section": to_next},
        )

    def hidden_copy(m):
        return pltpu.make_async_copy(hid.at[m], hidden_hbm.at[m], hid_sem.at[m])

    blocks = width // 128
    feature = lax.broadcasted_iota(jnp.int32, (1, 128), 1)

    @pl.loop(0, micro)
    def _(m):
        @pl.when(section > 0)
        def _():
            token_copy(m).wait_recv()

        alive = live_rows[m, 0:1, 0:rows]
        tokens = xin[m].astype(jnp.float32)
        normed = (normalised(tokens) * gain).astype(jnp.bfloat16)
        step = 640 if (3 * width) % 640 == 0 else 3 * width
        for c in range(0, 3 * width, step):
            qkv[:, c : c + step] = jnp.dot(
                normed, wqkv[:, c : c + step], preferred_element_type=jnp.float32
            ).astype(jnp.bfloat16)

        sums = [None] * blocks
        for h in range(heads):
            low, high = (h * HDIM, (h + 1) * HDIM)
            scores = None
            mine = range(low // 128, (high - 1) // 128 + 1)
            inside = {b: (feature >= low - 128 * b) & (feature < high - 128 * b) for b in mine}
            for b in mine:
                q = qkv[:, 128 * b : 128 * b + 128]
                q = jnp.where(inside[b], q, jnp.zeros_like(q))
                k = qkv[:, width + 128 * b : width + 128 * b + 128]
                term = lax.dot_general(
                    q, k, (((1,), (1,)), ((), ())), preferred_element_type=jnp.float32
                )
                scores = term if scores is None else scores + term
            scores = jnp.where(alive > 0.5, scores * HDIM ** (-0.5), -1e30)
            weights = jnp.exp(scores - jnp.max(scores, -1, keepdims=True))
            prob = (weights / jnp.sum(weights, -1, keepdims=True)).astype(jnp.bfloat16)
            for b in mine:
                v = qkv[:, 2 * width + 128 * b : 2 * width + 128 * b + 128]
                v = jnp.where(inside[b], v, jnp.zeros_like(v))
                term = jnp.dot(prob, v, preferred_element_type=jnp.float32)
                sums[b] = term if sums[b] is None else sums[b] + term
        for b in range(blocks):
            ctx[:, 128 * b : 128 * b + 128] = sums[b].astype(jnp.bfloat16)
        context = ctx[...]
        step = 640 if model % 640 == 0 else model
        for c in range(0, model, step):
            total = jnp.dot(context, wout[:, c : c + step], preferred_element_type=jnp.float32)
            total = total + xin[m, :, c : c + step].astype(jnp.float32)
            yout[m, :, c : c + step] = total.astype(jnp.bfloat16)

        @pl.when(section < last)
        def _():
            token_copy(m).start()

        live_column = column(alive)
        result = yout[m].astype(jnp.float32)
        hid[m] = jnp.where(live_column > 0.5, result, 0.0).astype(jnp.bfloat16)
        hidden_copy(m).start()
        deviation = normalised(result) - target[m].astype(jnp.float32)
        error = jnp.mean(deviation * deviation, -1, keepdims=True)
        error = jnp.where(live_column > 0.5, error, 0.0)
        error = jnp.sum(jnp.where(eye, error, 0.0), axis=0, keepdims=True)

        @pl.when(section > 0)
        def _():
            error_copy(m).wait_recv()

        err_out[m] = err_in[m] + jnp.broadcast_to(error, err_in.shape[1:])

        @pl.when(section < last)
        def _():
            error_copy(m).start()

    def total_copy(there):
        return pltpu.make_async_remote_copy(
            src_ref=tl.at[0],
            dst_ref=tl.at[1],
            send_sem=t_send.at[there],
            recv_sem=t_recv,
            device_id={"section": there},
        )

    @pl.when(section == last)
    def _():
        band = lax.broadcasted_iota(jnp.int32, (8, 128), 0)
        whole = jnp.zeros((8, 128), jnp.float32)
        for m in range(micro):
            whole = jnp.where(band == m, err_out[m], whole)
        tl[0] = whole
        tl[1] = whole
        for there in range(last):
            total_copy(there).start()

    @pl.when(section < last)
    def _():
        total_copy(section).wait_recv()

    band = lax.broadcasted_iota(jnp.int32, (8, 128), 0)
    whole = tl[1]
    token_ref[...] = whole[0:micro, 0:rows]
    own = jnp.broadcast_to(jnp.sum(whole, axis=1, keepdims=True), (8, 128))
    for m in range(micro):
        number = jnp.sum(live_rows[m, :, 0:rows], axis=1, keepdims=True)
        own = jnp.where(band == micro + m, number, own)
    part_own[...] = own
    slots_x[mx] = own

    def x_copy(there, slot):
        return pltpu.make_async_remote_copy(
            src_ref=part_own,
            dst_ref=slots_x.at[slot],
            send_sem=rx_send.at[there],
            recv_sem=rx_recv.at[slot],
            device_id={"dp": there * zs + mz},
        )

    def z_copy(there, slot):
        return pltpu.make_async_remote_copy(
            src_ref=part_mid,
            dst_ref=slots_z.at[slot],
            send_sem=rz_send.at[there],
            recv_sem=rz_recv.at[slot],
            device_id={"dp": mx * zs + there},
        )

    for k in range(1, xs):
        x_copy(lax.rem(mx + k, xs), mx).start()
    for k in range(1, xs):
        there = lax.rem(mx + k, xs)
        x_copy(there, there).wait_recv()
    mid = slots_x[0]
    for k in range(1, xs):
        mid = mid + slots_x[k]
    part_mid[...] = mid
    slots_z[mz] = mid
    for k in range(1, zs):
        z_copy(lax.rem(mz + k, zs), mz).start()
    for k in range(1, zs):
        there = lax.rem(mz + k, zs)
        z_copy(there, there).wait_recv()
    total = slots_z[0]
    for k in range(1, zs):
        total = total + slots_z[k]
    loss_ref[...] = total[0:micro] / total[micro : 2 * micro]

    for copy in sends:
        copy.wait_send()

    @pl.loop(0, micro)
    def _(m):
        hidden_copy(m).wait()

        @pl.when(section < last)
        def _():
            token_copy(m).wait_send()
            error_copy(m).wait_send()

    @pl.when(section == last)
    def _():
        for there in range(last):
            total_copy(there).wait_send()

    for k in range(1, xs):
        x_copy(lax.rem(mx + k, xs), mx).wait_send()
    for k in range(1, zs):
        z_copy(lax.rem(mz + k, zs), mz).wait_send()


def per_device(
    sections, xs, zs, patch_tokens, visible, keep_mask, lengths, qkv_weight, out_weight, norm_gain, targets
):
    micro, _, rows = visible.shape
    patches, model = patch_tokens.shape[2:]
    depth, columns = qkv_weight.shape[1:]
    odepth = out_weight.shape[1]
    heads = columns // (3 * HDIM)
    width = heads * HDIM
    devices = xs * zs
    dims = (sections, xs, zs, micro, rows, model, heads)
    bf, f32 = (jnp.bfloat16, jnp.float32)
    vmem = pl.BlockSpec(memory_space=pltpu.VMEM)
    hbm = pl.BlockSpec(memory_space=pl.ANY)
    dma = pltpu.SemaphoreType.DMA
    hidden, token, loss = pl.pallas_call(
        functools.partial(kernel, dims),
        out_shape=(
            jax.ShapeDtypeStruct((micro, rows, model), bf),
            jax.ShapeDtypeStruct((micro, rows), f32),
            jax.ShapeDtypeStruct((micro, 128), f32),
        ),
        in_specs=[pl.BlockSpec(memory_space=pltpu.SMEM)] + [vmem] * 5 + [hbm] * 2,
        out_specs=(hbm, vmem, vmem),
        scratch_shapes=[
            pltpu.VMEM((devices, depth * 2, model), bf),
            pltpu.VMEM((depth * devices, columns), bf),
            pltpu.VMEM((odepth * devices, model), bf),
            pltpu.VMEM((micro, patches, model), bf),
            pltpu.VMEM((micro, rows, model), bf),
            pltpu.VMEM((micro, rows, model), bf),
            pltpu.VMEM((micro, rows, model), bf),
            pltpu.VMEM((micro, rows, model), bf),
            pltpu.VMEM((rows, columns), bf),
            pltpu.VMEM((rows, width), bf),
            pltpu.VMEM((micro, 8, 128), f32),
            pltpu.VMEM((micro, 8, 128), f32),
            pltpu.VMEM((micro, 8, 128), f32),
            pltpu.VMEM((2, 8, 128), f32),
            pltpu.VMEM((8, 128), f32),
            pltpu.VMEM((8, 128), f32),
            pltpu.VMEM((xs, 8, 128), f32),
            pltpu.VMEM((zs, 8, 128), f32),
            dma((2,)),
            dma((micro,)),
            dma((2, devices)),
            dma((2, 2 * zs)),
            dma((2, 2 * zs, 2 * zs)),
            dma((micro,)),
            dma((micro,)),
            dma((micro,)),
            dma((micro,)),
            dma((sections,)),
            dma,
            dma((xs,)),
            dma((xs,)),
            dma((zs,)),
            dma((zs,)),
        ],
        compiler_params=pltpu.CompilerParams(collective_id=0, has_side_effects=True),
    )(
        lengths,
        visible[:, 0],
        keep_mask[:, 0],
        qkv_weight[0],
        out_weight[0],
        norm_gain,
        patch_tokens[:, 0],
        targets[0, :, 0],
    )
    return (hidden[None, :, None], token[:, None], loss[:, 0])


def solution(mesh):
    sections, devices = (mesh.shape["section"], mesh.shape["dp"])
    placed = (
        P(None, "dp", None, None),
        P(None, "dp", None),
        P(None, "dp", None),
        P(),
        P("section", "dp", None),
        P("section", "dp", None),
        P("section", None),
        P("section", None, "dp", None, None),
    )
    return jax.shard_map(
        functools.partial(per_device, sections, X, devices // X),
        mesh=mesh,
        in_specs=placed,
        out_specs=(P("section", None, "dp", None, None), P(None, "dp", None), P()),
        check_vma=False,
    )
```

```python
import functools

import jax
import jax.numpy as jnp
from jax import lax
from jax.experimental import pallas as pl
from jax.experimental.pallas import tpu as pltpu
from jax.sharding import PartitionSpec as P

HDIM = 80
SPLIT = 48
X = 4


def normalised(values):
    row_mean = jnp.mean(values, -1, keepdims=True)
    centered = values - row_mean
    variance = jnp.mean(centered * centered, -1, keepdims=True)
    return centered * lax.rsqrt(variance + 1e-06)


def gather_plan(xs, zs):
    waiting = []

    def one_way(part, where):
        out = []
        if part == 0:
            first, second = (zs, xs)
        else:
            first, second = (xs, zs)
        flows = {1: first // 2, -1: first - 1 - first // 2}
        cross = {1: second // 2, -1: second - 1 - second // 2}
        return (flows, cross)

    times = {}
    links = {}
    heap = []
    cost = {0: 2.6, 1: 1.8}

    def link_of(key, way, ring):
        part, f, s = key
        if ring == 0:
            sign = way
        else:
            sign = way if f % 2 == 0 else -way
        dim = ("z", "x")[part] if ring == 0 else ("x", "z")[part]
        return (dim, sign)

    def push(key, way, ring, ready):
        heap.append((ready, len(heap), key, way, ring))

    def arrived(key, ready):
        part, f, s = key
        flows, cross = one_way(part, None)
        if s == 0:
            for way in (1, -1):
                if (f == 0 or (f > 0) == (way > 0)) and abs(f) < flows[way]:
                    push((part, f + way, 0), way, 0, ready)
            for way in (1, -1):
                push((part, f, way), way, 1, ready + 0.01)
        else:
            way = 1 if s > 0 else -1
            if abs(s) < cross[way]:
                push((part, f, s + way), way, 1, ready)

    arrived((0, 0, 0), 0.0)
    arrived((1, 0, 0), 0.0)
    while heap:
        heap.sort()
        ready, _, key, way, ring = heap.pop(0)
        link = link_of(key, way, ring)
        begin = max(ready, links.get(link, 0.0))
        links[link] = begin + cost[key[0]]
        times[key] = begin + cost[key[0]] + 1.6
        arrived(key, times[key] + 0.1)
    return sorted(times, key=lambda key: times[key])


def kernel(
    dims,
    lengths_ref,
    visible_ref,
    keep_ref,
    wq_ref,
    wo_ref,
    gain_ref,
    patch_hbm,
    target_hbm,
    hidden_hbm,
    token_ref,
    loss_ref,
    slabs,
    wqkv,
    wout,
    patch,
    target,
    xin,
    yout,
    hid,
    qkv,
    ctx,
    err_in,
    err_out,
    live_rows,
    tl,
    part_own,
    part_mid,
    slots_x,
    slots_z,
    load_sem,
    hid_sem,
    own_recv,
    slab_send,
    x_send,
    x_recv,
    e_send,
    e_recv,
    t_send,
    t_recv,
    rx_send,
    rx_recv,
    rz_send,
    rz_recv,
):
    sections, xs, zs, micro, rows, model, heads = dims
    width = heads * HDIM
    patches = patch.shape[1]
    section = lax.axis_index("section")
    me = lax.axis_index("dp")
    mx, mz = me // zs, me % zs
    last = sections - 1
    ring = {"x": xs, "z": zs}

    def at(x, z):
        return lax.rem(x + 2 * xs, xs) * zs + lax.rem(z + 2 * zs, zs)

    barrier = pltpu.get_barrier_semaphore()
    for there in (at(mx + 1, mz), at(mx - 1, mz), at(mx, mz + 1), at(mx, mz - 1)):
        pl.semaphore_signal(barrier, inc=1, device_id={"dp": there})

    @pl.when(section > 0)
    def _():
        pl.semaphore_signal(barrier, inc=1, device_id={"section": section - 1})

    @pl.when(section < last)
    def _():
        pl.semaphore_signal(barrier, inc=1, device_id={"section": section + 1})

    target_load = pltpu.make_async_copy(target_hbm, target, load_sem.at[0])
    target_load.start()
    patch_load = pltpu.make_async_copy(patch_hbm, patch, load_sem.at[1])
    patch_load.start()

    half = model // 2
    w = wq_ref[...].astype(jnp.float32)
    o = wo_ref[...].astype(jnp.float32)
    left = jnp.concatenate(
        [
            w[:, :half],
            w[0:8, model : model + half],
            w[16:24, model : model + half],
            w[32:40, model : model + half],
            o[0:16, :half],
        ],
        axis=0,
    )
    right = jnp.concatenate(
        [
            w[:, half:model],
            w[8:16, model : model + half],
            w[24:32, model : model + half],
            jnp.concatenate([o[16:20, :half], o[16:20, half:]], axis=0),
            o[0:16, half:],
        ],
        axis=0,
    )
    slabs[me, :, 0:half] = left.astype(jnp.bfloat16)
    slabs[me, :, half:model] = right.astype(jnp.bfloat16)

    pl.semaphore_wait(barrier, 4 + jnp.minimum(section, 1) + jnp.minimum(last - section, 1))

    def sign(c):
        return 1 - 2 * lax.rem(c + 2 * xs * zs, 2)

    def cut(origin, part):
        if part == 0:
            return slabs.at[origin, pl.ds(0, SPLIT)]
        return slabs.at[origin, pl.ds(SPLIT, slabs.shape[1] - SPLIT)]

    def place(key, receiver):
        part, f, s = key
        if part == 0:
            way1 = sign(mx)
            if receiver:
                oz = mz - f * way1
                way2 = sign(oz)
                return at(mx - s * way2, oz), None
        else:
            way1 = sign(mz)
            if receiver:
                ox = mx - f * way1
                way2 = sign(ox)
                return at(ox, mz - s * way2), None

    def send(key):
        part, f, s = key
        step = 1 if (s > 0 or (s == 0 and f > 0)) else -1
        if part == 0:
            way1 = sign(mx)
            if s == 0:
                origin = at(mx, mz - (f - step) * way1)
                there = at(mx, mz + step * way1)
            else:
                oz = mz - f * way1
                way2 = sign(oz)
                origin = at(mx - (s - step) * way2, oz)
                there = at(mx + step * way2, mz)
        else:
            way1 = sign(mz)
            if s == 0:
                origin = at(mx - (f - step) * way1, mz)
                there = at(mx + step * way1, mz)
            else:
                ox = mx - f * way1
                way2 = sign(ox)
                origin = at(ox, mz - (s - step) * way2)
                there = at(mx, mz + step * way2)
        copy = pltpu.make_async_remote_copy(
            src_ref=cut(origin, part),
            dst_ref=cut(origin, part),
            send_sem=slab_send,
            recv_sem=own_recv.at[part, origin],
            device_id={"dp": there},
        )
        copy.start()

    def after(key):
        part, f, s = key
        first, second = (zs, xs) if part == 0 else (xs, zs)
        flows = {1: first // 2, -1: first - 1 - first // 2}
        cross = {1: second // 2, -1: second - 1 - second // 2}
        if s == 0:
            for way in (1, -1):
                if (f == 0 or (f > 0) == (way > 0)) and abs(f) < flows[way]:
                    send((part, f + way, 0))
            for way in (1, -1):
                send((part, f, way))
        else:
            way = 1 if s > 0 else -1
            if abs(s) < cross[way]:
                send((part, f, s + way))

    plan = gather_plan(xs, zs)
    after((0, 0, 0))
    after((1, 0, 0))

    lane = lax.broadcasted_iota(jnp.int32, (rows, 128), 1)
    sub = lax.broadcasted_iota(jnp.int32, (rows, 128), 0)
    eye = lane == sub
    slot = lax.broadcasted_iota(jnp.int32, (1, rows), 1)
    for m in range(micro):
        keep = keep_ref[m : m + 1, :]
        alive = jnp.where((slot < lengths_ref[m]) & (keep == 1), 1.0, 0.0)
        live_rows[m, :, 0:rows] = jnp.broadcast_to(alive, (8, rows))

    def column(row):
        return jnp.sum(jnp.where(eye[:, :rows], row, 0.0), axis=1, keepdims=True)

    patch_load.wait()

    @pl.when(section == 0)
    def _():
        for m in range(micro):
            chosen = column(visible_ref[m : m + 1, :].astype(jnp.float32))
            spot = lax.broadcasted_iota(jnp.int32, (rows, patches), 1).astype(jnp.float32)
            pick = jnp.where(spot == chosen, 1.0, 0.0).astype(jnp.bfloat16)
            xin[m] = jnp.dot(pick, patch[m], preferred_element_type=jnp.float32).astype(
                jnp.bfloat16
            )
            err_in[m] = jnp.zeros(err_in.shape[1:], jnp.float32)

    for key in plan:
        part = key[0]
        origin, _ = place(key, True)
        pltpu.make_async_remote_copy(
            src_ref=cut(origin, part),
            dst_ref=cut(origin, part),
            send_sem=slab_send,
            recv_sem=own_recv.at[part, origin],
            device_id={"dp": me},
        ).wait_recv()
        after(key)

    @pl.loop(0, xs * zs // 4)
    def _(g):
        r160 = pl.multiple_of(g * 160, 16)
        r80 = pl.multiple_of(g * 80, 16)
        for c in range(0, half, 128):
            a = [slabs[g * 4 + j, :, c : c + 128].astype(jnp.float32) for j in range(4)]
            b = [
                slabs[g * 4 + j, :, half + c : half + c + 128].astype(jnp.float32)
                for j in range(4)
            ]
            qk0 = jnp.concatenate([t[0:40] for t in a], axis=0)
            qk1 = jnp.concatenate([t[0:40] for t in b], axis=0)
            val = []
            o0 = []
            o1 = []
            for t, u in zip(a, b):
                val += [t[40:48], u[40:48], t[48:56], u[48:56], t[56:64]]
                o0 += [t[64:80], u[56:60]]
                o1 += [u[64:80], u[60:64]]
            wqkv[pl.ds(r160, 160), c : c + 128] = qk0.astype(jnp.bfloat16)
            wqkv[pl.ds(r160, 160), half + c : half + c + 128] = qk1.astype(jnp.bfloat16)
            wqkv[pl.ds(r160, 160), model + c : model + c + 128] = jnp.concatenate(
                val, axis=0
            ).astype(jnp.bfloat16)
            wout[pl.ds(r80, 80), c : c + 128] = jnp.concatenate(o0, axis=0).astype(jnp.bfloat16)
            wout[pl.ds(r80, 80), half + c : half + c + 128] = jnp.concatenate(
                o1, axis=0
            ).astype(jnp.bfloat16)

    target_load.wait()
    gain = gain_ref[...].astype(jnp.float32)
    to_next = jnp.minimum(section + 1, last)

    def token_copy(m, i):
        piece = pl.ds(i * half, half)
        return pltpu.make_async_remote_copy(
            src_ref=yout.at[m, :, piece],
            dst_ref=xin.at[m, :, piece],
            send_sem=x_send.at[m, i],
            recv_sem=x_recv.at[m, i],
            device_id={"section": to_next},
        )

    def error_copy(m):
        return pltpu.make_async_remote_copy(
            src_ref=err_out.at[m],
            dst_ref=err_in.at[m],
            send_sem=e_send.at[m],
            recv_sem=e_recv.at[m],
            device_id={"section": to_next},
        )

    def hidden_copy(m):
        return pltpu.make_async_copy(hid.at[m], hidden_hbm.at[m], hid_sem.at[m])

    blocks = width // 128
    feature = lax.broadcasted_iota(jnp.int32, (1, 128), 1)

    @pl.loop(0, micro)
    def _(m):
        @pl.when(section > 0)
        def _():
            token_copy(m, 0).wait_recv()
            token_copy(m, 1).wait_recv()

        alive = live_rows[m, 0:1, 0:rows]
        tokens = xin[m].astype(jnp.float32)
        normed = (normalised(tokens) * gain).astype(jnp.bfloat16)
        step = 640 if (3 * width) % 640 == 0 else 3 * width
        for c in range(0, 3 * width, step):
            qkv[:, c : c + step] = jnp.dot(
                normed, wqkv[:, c : c + step], preferred_element_type=jnp.float32
            ).astype(jnp.bfloat16)

        sums = [None] * blocks
        for h in range(heads):
            low, high = (h * HDIM, (h + 1) * HDIM)
            scores = None
            mine = range(low // 128, (high - 1) // 128 + 1)
            inside = {b: (feature >= low - 128 * b) & (feature < high - 128 * b) for b in mine}
            for b in mine:
                q = qkv[:, 128 * b : 128 * b + 128]
                q = jnp.where(inside[b], q, jnp.zeros_like(q))
                k = qkv[:, width + 128 * b : width + 128 * b + 128]
                term = lax.dot_general(
                    q, k, (((1,), (1,)), ((), ())), preferred_element_type=jnp.float32
                )
                scores = term if scores is None else scores + term
            scores = jnp.where(alive > 0.5, scores * HDIM ** (-0.5), -1e30)
            weights = jnp.exp(scores - jnp.max(scores, -1, keepdims=True))
            prob = (weights / jnp.sum(weights, -1, keepdims=True)).astype(jnp.bfloat16)
            for b in mine:
                v = qkv[:, 2 * width + 128 * b : 2 * width + 128 * b + 128]
                v = jnp.where(inside[b], v, jnp.zeros_like(v))
                term = jnp.dot(prob, v, preferred_element_type=jnp.float32)
                sums[b] = term if sums[b] is None else sums[b] + term
        for b in range(blocks):
            ctx[:, 128 * b : 128 * b + 128] = sums[b].astype(jnp.bfloat16)
        context = ctx[...]
        for i in range(2):
            c = i * half
            total = jnp.dot(context, wout[:, c : c + half], preferred_element_type=jnp.float32)
            total = total + xin[m, :, c : c + half].astype(jnp.float32)
            yout[m, :, c : c + half] = total.astype(jnp.bfloat16)

            @pl.when(section < last)
            def _():
                token_copy(m, i).start()

        live_column = column(alive)
        result = yout[m].astype(jnp.float32)
        hid[m] = jnp.where(live_column > 0.5, result, 0.0).astype(jnp.bfloat16)
        hidden_copy(m).start()
        deviation = normalised(result) - target[m].astype(jnp.float32)
        error = jnp.mean(deviation * deviation, -1, keepdims=True)
        error = jnp.where(live_column > 0.5, error, 0.0)
        error = jnp.sum(jnp.where(eye, error, 0.0), axis=0, keepdims=True)

        @pl.when(section > 0)
        def _():
            error_copy(m).wait_recv()

        err_out[m] = err_in[m] + jnp.broadcast_to(error, err_in.shape[1:])

        @pl.when(section < last)
        def _():
            error_copy(m).start()

    def total_copy(there):
        return pltpu.make_async_remote_copy(
            src_ref=tl.at[0],
            dst_ref=tl.at[1],
            send_sem=t_send.at[there],
            recv_sem=t_recv,
            device_id={"section": there},
        )

    @pl.when(section == last)
    def _():
        band = lax.broadcasted_iota(jnp.int32, (8, 128), 0)
        whole = jnp.zeros((8, 128), jnp.float32)
        for m in range(micro):
            whole = jnp.where(band == m, err_out[m], whole)
        tl[0] = whole
        tl[1] = whole
        for there in range(last):
            total_copy(there).start()

    @pl.when(section < last)
    def _():
        total_copy(section).wait_recv()

    band = lax.broadcasted_iota(jnp.int32, (8, 128), 0)
    whole = tl[1]
    token_ref[...] = whole[0:micro, 0:rows]
    own = jnp.broadcast_to(jnp.sum(whole, axis=1, keepdims=True), (8, 128))
    for m in range(micro):
        number = jnp.sum(live_rows[m, :, 0:rows], axis=1, keepdims=True)
        own = jnp.where(band == micro + m, number, own)
    part_own[...] = own
    slots_x[mx] = own

    def x_copy(there, slot):
        return pltpu.make_async_remote_copy(
            src_ref=part_own,
            dst_ref=slots_x.at[slot],
            send_sem=rx_send.at[there],
            recv_sem=rx_recv.at[slot],
            device_id={"dp": there * zs + mz},
        )

    def z_copy(there, slot):
        return pltpu.make_async_remote_copy(
            src_ref=part_mid,
            dst_ref=slots_z.at[slot],
            send_sem=rz_send.at[there],
            recv_sem=rz_recv.at[slot],
            device_id={"dp": mx * zs + there},
        )

    for k in range(1, xs):
        x_copy(lax.rem(mx + k, xs), mx).start()
    for k in range(1, xs):
        there = lax.rem(mx + k, xs)
        x_copy(there, there).wait_recv()
    mid = slots_x[0]
    for k in range(1, xs):
        mid = mid + slots_x[k]
    part_mid[...] = mid
    slots_z[mz] = mid
    for k in range(1, zs):
        z_copy(lax.rem(mz + k, zs), mz).start()
    for k in range(1, zs):
        there = lax.rem(mz + k, zs)
        z_copy(there, there).wait_recv()
    total = slots_z[0]
    for k in range(1, zs):
        total = total + slots_z[k]
    loss_ref[...] = total[0:micro] / total[micro : 2 * micro]

    others = slabs.at[pl.ds(0, xs * zs - 1)]
    pltpu.make_async_remote_copy(
        src_ref=others,
        dst_ref=others,
        send_sem=slab_send,
        recv_sem=t_recv,
        device_id={"dp": me},
    ).wait_send()

    @pl.loop(0, micro)
    def _(m):
        hidden_copy(m).wait()

        @pl.when(section < last)
        def _():
            token_copy(m, 0).wait_send()
            token_copy(m, 1).wait_send()
            error_copy(m).wait_send()

    @pl.when(section == last)
    def _():
        for there in range(last):
            total_copy(there).wait_send()

    for k in range(1, xs):
        x_copy(lax.rem(mx + k, xs), mx).wait_send()
    for k in range(1, zs):
        z_copy(lax.rem(mz + k, zs), mz).wait_send()


def per_device(
    sections, xs, zs, patch_tokens, visible, keep_mask, lengths, qkv_weight, out_weight, norm_gain, targets
):
    micro, _, rows = visible.shape
    patches, model = patch_tokens.shape[2:]
    depth, columns = qkv_weight.shape[1:]
    odepth = out_weight.shape[1]
    heads = columns // (3 * HDIM)
    width = heads * HDIM
    devices = xs * zs
    dims = (sections, xs, zs, micro, rows, model, heads)
    bf, f32 = (jnp.bfloat16, jnp.float32)
    vmem = pl.BlockSpec(memory_space=pltpu.VMEM)
    hbm = pl.BlockSpec(memory_space=pl.ANY)
    dma = pltpu.SemaphoreType.DMA
    hidden, token, loss = pl.pallas_call(
        functools.partial(kernel, dims),
        out_shape=(
            jax.ShapeDtypeStruct((micro, rows, model), bf),
            jax.ShapeDtypeStruct((micro, rows), f32),
            jax.ShapeDtypeStruct((micro, 128), f32),
        ),
        in_specs=[pl.BlockSpec(memory_space=pltpu.SMEM)] + [vmem] * 5 + [hbm] * 2,
        out_specs=(hbm, vmem, vmem),
        scratch_shapes=[
            pltpu.VMEM((devices, depth * 2, model), bf),
            pltpu.VMEM((depth * devices, columns), bf),
            pltpu.VMEM((odepth * devices, model), bf),
            pltpu.VMEM((micro, patches, model), bf),
            pltpu.VMEM((micro, rows, model), bf),
            pltpu.VMEM((micro, rows, model), bf),
            pltpu.VMEM((micro, rows, model), bf),
            pltpu.VMEM((micro, rows, model), bf),
            pltpu.VMEM((rows, columns), bf),
            pltpu.VMEM((rows, width), bf),
            pltpu.VMEM((micro, 8, 128), f32),
            pltpu.VMEM((micro, 8, 128), f32),
            pltpu.VMEM((micro, 8, 128), f32),
            pltpu.VMEM((2, 8, 128), f32),
            pltpu.VMEM((8, 128), f32),
            pltpu.VMEM((8, 128), f32),
            pltpu.VMEM((xs, 8, 128), f32),
            pltpu.VMEM((zs, 8, 128), f32),
            dma((2,)),
            dma((micro,)),
            dma((2, devices)),
            dma,
            dma((micro, 2)),
            dma((micro, 2)),
            dma((micro,)),
            dma((micro,)),
            dma((sections,)),
            dma,
            dma((xs,)),
            dma((xs,)),
            dma((zs,)),
            dma((zs,)),
        ],
        compiler_params=pltpu.CompilerParams(collective_id=0, has_side_effects=True),
    )(
        lengths,
        visible[:, 0],
        keep_mask[:, 0],
        qkv_weight[0],
        out_weight[0],
        norm_gain,
        patch_tokens[:, 0],
        targets[0, :, 0],
    )
    return (hidden[None, :, None], token[:, None], loss[:, 0])


def solution(mesh):
    sections, devices = (mesh.shape["section"], mesh.shape["dp"])
    placed = (
        P(None, "dp", None, None),
        P(None, "dp", None),
        P(None, "dp", None),
        P(),
        P("section", "dp", None),
        P("section", "dp", None),
        P("section", None),
        P("section", None, "dp", None, None),
    )
    return jax.shard_map(
        functools.partial(per_device, sections, X, devices // X),
        mesh=mesh,
        in_specs=placed,
        out_specs=(P("section", None, "dp", None, None), P(None, "dp", None), P()),
        check_vma=False,
    )
```
